128 devices in a mesh: data: 1, tp: 64 (over z, y, x), ep: 2 (over core).
Axes of the slice: x: 4, y: 4, z: 4, core: 2. Of those that a mesh axis runs over, the one named last changes fastest.
Arguments:
- tokens_a: bfloat16 [4096, 2048], P(('data', 'ep', 'tp'))
- tokens_b: bfloat16 [4096, 2048], P(('data', 'ep', 'tp'))
- experts_a: int32 [4096, 4], P(('data', 'ep', 'tp'))
- experts_b: int32 [4096, 4], P(('data', 'ep', 'tp'))
- gates_a: float32 [4096, 4], P(('data', 'ep', 'tp'))
- gates_b: float32 [4096, 4], P(('data', 'ep', 'tp'))
- slots_a: int32 [4096, 4], P(('data', 'ep', 'tp'))
- slots_b: int32 [4096, 4], P(('data', 'ep', 'tp'))
- shared_w1: bfloat16 [2048, 5632], P(None, 'tp')
- shared_w3: bfloat16 [2048, 5632], P(None, 'tp')
- shared_w2: bfloat16 [5632, 2048], P('tp')
- routed_w1: bfloat16 [60, 2048, 1408], P('ep')
- routed_w3: bfloat16 [60, 2048, 1408], P('ep')
- routed_w2: bfloat16 [60, 1408, 2048], P('ep')
Outputs:
- output 1: bfloat16 [4096, 2048], P(('data', 'ep', 'tp'))
- output 2: bfloat16 [4096, 2048], P(('data', 'ep', 'tp'))
All inputs are finite; a program needn't handle non-finite values.
Results may differ from the reference program's by a relative error of at most 0.0049404.
Values are sent between devices in bfloat16 or wider.
A program may use at most 1.5 GiB of HBM per device.

```python
import jax
import jax.numpy as jnp
from jax import lax

TOK_DEV = 32
TP_SIZE = 64
EP_SIZE = 2
MODEL_DIM = 2048
EXPERTS = 60
TOP_K = 4
EXPERT_FF = 1408
SHARED_FF = 5632
CAPACITY = 4

GROUP_DEVS = TP_SIZE * EP_SIZE
GROUP_TOK = GROUP_DEVS * TOK_DEV


def draw_routing(key):
    key_base, key_rank, key_tie = jax.random.split(key, 3)
    base = jax.random.randint(key_base, (GROUP_TOK, EXPERTS), 0, 64)
    rank_of = jax.random.permutation(key_rank, EXPERTS)
    favoured = jnp.where((rank_of >= 1) & (rank_of <= EXPERTS // 8), 6, 0)
    forced = jnp.where(rank_of == 0, 4096, 0)
    tok_ids = jnp.arange(GROUP_TOK)
    head_tok = (tok_ids % TOK_DEV) < CAPACITY
    cover = jnp.where(tok_ids[:, None] == jnp.arange(EXPERTS)[None, :], 4096, 0)
    score = base + favoured[None, :] + jnp.where(head_tok[:, None], forced[None, :], 0) + cover
    tie_rank = jax.random.permutation(key_tie, jnp.broadcast_to(jnp.arange(EXPERTS), (GROUP_TOK, EXPERTS)), axis=1, independent=True)
    chosen = lax.top_k(score * EXPERTS + tie_rank, TOP_K)[1]
    per_dev = chosen.reshape(GROUP_DEVS, TOK_DEV * TOP_K)
    one_hot = (per_dev[:, :, None] == jnp.arange(EXPERTS)[None, None, :]).astype(jnp.int32)
    earlier = jnp.cumsum(one_hot, axis=1) - one_hot
    position = jnp.sum(earlier * one_hot, axis=2)
    slots = jnp.where(position < CAPACITY, position, -1).reshape(GROUP_TOK, TOP_K)
    return chosen.astype(jnp.int32), slots.astype(jnp.int32)


def setup_inputs(seed: int = 0, part: int = 0) -> dict:
    key = jax.random.key(seed)
    part_keys = jax.random.split(jax.random.fold_in(key, part), 6)
    weight_keys = jax.random.split(key, 6)
    tokens_a = jax.random.normal(part_keys[0], (GROUP_TOK, MODEL_DIM), jnp.float32).astype(jnp.bfloat16)
    tokens_b = jax.random.normal(part_keys[1], (GROUP_TOK, MODEL_DIM), jnp.float32).astype(jnp.bfloat16)
    experts_a, slots_a = draw_routing(part_keys[2])
    experts_b, slots_b = draw_routing(part_keys[3])
    gates_a = jax.random.uniform(part_keys[4], (GROUP_TOK, TOP_K), jnp.float32, 0.5, 1.5) * TOP_K ** -0.5
    gates_b = jax.random.uniform(part_keys[5], (GROUP_TOK, TOP_K), jnp.float32, 0.5, 1.5) * TOP_K ** -0.5
    shared_w1 = (jax.random.normal(weight_keys[0], (MODEL_DIM, SHARED_FF), jnp.float32) * MODEL_DIM ** -0.5).astype(jnp.bfloat16)
    shared_w3 = (jax.random.normal(weight_keys[1], (MODEL_DIM, SHARED_FF), jnp.float32) * MODEL_DIM ** -0.5).astype(jnp.bfloat16)
    shared_w2 = (jax.random.normal(weight_keys[2], (SHARED_FF, MODEL_DIM), jnp.float32) * SHARED_FF ** -0.5).astype(jnp.bfloat16)
    routed_w1 = (jax.random.normal(weight_keys[3], (EXPERTS, MODEL_DIM, EXPERT_FF), jnp.float32) * MODEL_DIM ** -0.5).astype(jnp.bfloat16)
    routed_w3 = (jax.random.normal(weight_keys[4], (EXPERTS, MODEL_DIM, EXPERT_FF), jnp.float32) * MODEL_DIM ** -0.5).astype(jnp.bfloat16)
    routed_w2 = (jax.random.normal(weight_keys[5], (EXPERTS, EXPERT_FF, MODEL_DIM), jnp.float32) * EXPERT_FF ** -0.5).astype(jnp.bfloat16)
    return {'tokens_a': tokens_a, 'tokens_b': tokens_b, 'experts_a': experts_a, 'experts_b': experts_b, 'gates_a': gates_a, 'gates_b': gates_b, 'slots_a': slots_a, 'slots_b': slots_b, 'shared_w1': shared_w1, 'shared_w3': shared_w3, 'shared_w2': shared_w2, 'routed_w1': routed_w1, 'routed_w3': routed_w3, 'routed_w2': routed_w2}


def swiglu_rows(rows, w_in, w_gate, w_out):
    proj_in = jnp.dot(rows, w_in, preferred_element_type=jnp.float32)
    proj_gate = jnp.dot(rows, w_gate, preferred_element_type=jnp.float32)
    hidden = (jax.nn.silu(proj_in) * proj_gate).astype(jnp.bfloat16)
    return jnp.dot(hidden, w_out, preferred_element_type=jnp.float32)


def shared_expert(tokens, shared_w1, shared_w3, shared_w2):
    blocks = tokens.reshape(GROUP_DEVS, TOK_DEV, MODEL_DIM)
    result = lax.map(lambda token_block: swiglu_rows(token_block, shared_w1, shared_w3, shared_w2), blocks)
    return result.reshape(GROUP_TOK, MODEL_DIM)


def routed_experts(tokens, experts, gates, slots, routed_w1, routed_w3, routed_w2):
    tok_dev = tokens.reshape(GROUP_DEVS, TOK_DEV, MODEL_DIM).astype(jnp.float32)
    expert_dev = experts.reshape(GROUP_DEVS, TOK_DEV, TOP_K)
    slot_dev = slots.reshape(GROUP_DEVS, TOK_DEV, TOP_K)
    gate_dev = gates.reshape(GROUP_DEVS, TOK_DEV, TOP_K)
    slot_range = jnp.arange(CAPACITY)

    def one_expert(routed_acc, step_in):
        w_in, w_gate, w_out, expert = step_in
        hits = ((expert_dev == expert)[..., None] & (slot_dev[..., None] == slot_range)).astype(jnp.float32)
        place_mat = jnp.sum(hits, axis=2)
        gate_mat = jnp.sum(hits * gate_dev[..., None], axis=2)
        buffer_rows = jnp.einsum('ntc,ntd->ncd', place_mat, tok_dev).astype(jnp.bfloat16)
        expert_out = swiglu_rows(buffer_rows.reshape(GROUP_DEVS * CAPACITY, MODEL_DIM), w_in, w_gate, w_out).astype(jnp.bfloat16)
        expert_out = expert_out.reshape(GROUP_DEVS, CAPACITY, MODEL_DIM).astype(jnp.float32)
        return routed_acc + jnp.einsum('ntc,ncd->ntd', gate_mat, expert_out), None

    start_acc = jnp.zeros((GROUP_DEVS, TOK_DEV, MODEL_DIM), jnp.float32)
    routed_acc, unused = lax.scan(one_expert, start_acc, (routed_w1, routed_w3, routed_w2, jnp.arange(EXPERTS)))
    return routed_acc.reshape(GROUP_TOK, MODEL_DIM)


def one_microbatch(tokens, experts, gates, slots, shared_w1, shared_w3, shared_w2, routed_w1, routed_w3, routed_w2):
    shared_out = shared_expert(tokens, shared_w1, shared_w3, shared_w2)
    routed_out = routed_experts(tokens, experts, gates, slots, routed_w1, routed_w3, routed_w2)
    return (tokens.astype(jnp.float32) + shared_out + routed_out).astype(jnp.bfloat16)


def reference(tokens_a, tokens_b, experts_a, experts_b, gates_a, gates_b, slots_a, slots_b, shared_w1, shared_w3, shared_w2, routed_w1, routed_w3, routed_w2):
    out_a = one_microbatch(tokens_a, experts_a, gates_a, slots_a, shared_w1, shared_w3, shared_w2, routed_w1, routed_w3, routed_w2)
    out_b = one_microbatch(tokens_b, experts_b, gates_b, slots_b, shared_w1, shared_w3, shared_w2, routed_w1, routed_w3, routed_w2)
    return (out_a, out_b)
```

```python
import functools

import jax
import jax.numpy as jnp
from jax import lax
from jax.experimental import pallas as pl
from jax.experimental.pallas import tpu as pltpu
from jax.sharding import PartitionSpec as P

MESH = pl.DeviceIdType.MESH
BF16 = jnp.bfloat16
F32 = jnp.float32
LANES = 128
CHUNK = 256
STRIDE = (1, 4, 16)
SIDE = 4
CUBE = 8
HALF = 48


def capacity_rows(tok_local, top_k, num_experts):
    return max(4, (2 * tok_local * top_k) // num_experts)


def column_parts(width, order):
    tiles = width // LANES
    size = [tiles // 3] * 3
    for i in range(tiles % 3):
        size[order[i]] += 1
    starts = [0, size[0], size[0] + size[1]]
    return [(s * LANES, n * LANES) for s, n in zip(starts, size) if True]


def weight_of(t):
    return 4 - 2 * t + (t * (t - 1)) // 2


def kernel(cfg, ta, tb, ma, mb, w1, w3, w2, rw1, rw3, rw2, oa, ob,
           xg, wg13, wg2, h, hs, gm, rd, r1, r2, r3,
           loc_sem, wl_sem, w2_sem, ag_s, ag_r, g13_s, g13_r, g2_s, g2_r, xd_s, xd_r, rd_s, rd_r, rs_s, rs_r):
    tok, dim, ff, sff, n_local, cap, width = (cfg[k] for k in ("tok", "dim", "ff", "sff", "n_local", "cap", "width"))
    experts_here = cfg["experts_here"]
    n_chunks = dim // CHUNK
    per_chunk = CHUNK // LANES
    xcols = column_parts(dim + LANES, (0, 2, 1))
    wcols = column_parts(dim, (1, 0, 2))

    tp = lax.axis_index("tp")
    core = lax.axis_index("ep")
    coord = [tp % SIDE, (tp // SIDE) % SIDE, tp // (SIDE * SIDE)]
    near = [[tp + (1 - 2 * (c % 2)) * s for c, s in zip(coord, STRIDE)],
            [tp + (3 - 2 * c) * s for c, s in zip(coord, STRIDE)]]
    place = coord[0] % 2 + 2 * (coord[1] % 2) + 4 * (coord[2] % 2)

    def at(chip):
        return {"tp": chip, "ep": core}

    partner = {"tp": tp, "ep": 1 - core}

    def token_chip(m, d):
        n0, n1, n2 = near[m]
        return n0 + d * (n1 - n0) + ((d * (d - 1)) // 2) * (n2 - 2 * n1 + n0)

    def remote(src, dst, s, r, where):
        return pltpu.make_async_remote_copy(src_ref=src, dst_ref=dst, send_sem=s, recv_sem=r, device_id=where, device_id_type=MESH)

    def items_of(p, s):
        got = [0]
        for t in range(s):
            got = got + [i | (1 << ((p + t) % 3)) for i in got]
        return got

    def x_copy(m, p, s, i):
        d = (p + s) % 3
        to = i | (1 << d)
        c0, n = xcols[p]
        return remote(xg.at[m, pl.ds(i * tok, tok), pl.ds(c0, n)], xg.at[m, pl.ds(to * tok, tok), pl.ds(c0, n)],
                      ag_s.at[m, p, to], ag_r.at[m, p, to], at(near[m][d]))

    def w13_copy(m, p, s, i):
        d = (p + s) % 3
        to = i | (1 << d)
        c0, n = wcols[p]
        return remote(wg13.at[m, :, pl.ds(i * HALF, HALF), pl.ds(c0, n)], wg13.at[m, :, pl.ds(to * HALF, HALF), pl.ds(c0, n)],
                      g13_s.at[m, p, to], g13_r.at[m, p, to], at(near[1 - m][d]))

    def w2_copy(m, p, s, i):
        d = (p + s) % 3
        to = i | (1 << d)
        c0, n = wcols[p]
        return remote(wg2.at[m, pl.ds(i * HALF, HALF), pl.ds(c0, n)], wg2.at[m, pl.ds(to * HALF, HALF), pl.ds(c0, n)],
                      g2_s.at[m, p, to], g2_r.at[m, p, to], at(near[1 - m][d]))

    def step(copy, s, what):
        for m in range(2):
            for p in range(3):
                for i in items_of(p, s):
                    c = copy(m, p, s, i)
                    if what == "start":
                        c.start()
                    elif what == "recv":
                        c.wait_recv()
                    else:
                        c.wait_send()

    half_rows = CUBE * tok

    def x_swap(m):
        return remote(xg.at[m, pl.ds(0, half_rows)], xg.at[m, pl.ds(half_rows, half_rows)], xd_s.at[m], xd_r.at[m], partner)

    barrier = pltpu.get_barrier_semaphore()
    for kind in range(2):
        for d in range(3):
            pl.semaphore_signal(barrier, inc=1, device_id=at(near[kind][d]), device_id_type=MESH)
    pl.semaphore_signal(barrier, inc=1, device_id=partner, device_id_type=MESH)

    own = []
    for m, (t, meta) in enumerate(((ta, ma), (tb, mb))):
        own.append(pltpu.make_async_copy(t, xg.at[m, pl.ds(0, tok), pl.ds(0, dim)], loc_sem.at[2 * m]))
        own.append(pltpu.make_async_copy(meta, xg.at[m, pl.ds(0, tok), pl.ds(dim, LANES)], loc_sem.at[2 * m + 1]))

    def expert_row(j):
        return (place + CUBE * j) % n_local

    def first_stage(slots, xe, wt1, wt3, wt2):
        shared_in = [pltpu.make_async_copy(src, dst, loc_sem.at[4 + k]) for k, (src, dst) in enumerate(((w1, wt1), (w3, wt3), (w2, wt2)))]

        def routed_in(j):
            e = expert_row(j)
            slot = j % 2
            return [pltpu.make_async_copy(src.at[e], slots.at[slot, k], wl_sem.at[slot, k]) for k, src in enumerate((rw1, rw3))]

        for c in own + shared_in:
            c.start()
        for j in range(2):
            for c in routed_in(j):
                c.start()

        row = lax.broadcasted_iota(jnp.int32, (HALF, sff), 0)
        col = lax.broadcasted_iota(jnp.int32, (HALF, sff), 1)
        pick = (col == row + HALF * core).astype(BF16)
        for c in own:
            c.wait()
        for k, src in enumerate((wt1, wt3)):
            shared_in[k].wait()
            mine = lax.dot_general(pick, src[...], (((1,), (1,)), ((), ())), preferred_element_type=F32).astype(BF16)
            for m in range(2):
                wg13[m, k, 0:HALF, :] = mine
        shared_in[2].wait()
        mine = jnp.dot(pick, wt2[...], preferred_element_type=F32).astype(BF16)
        for m in range(2):
            wg2[m, 0:HALF, :] = mine

        pl.semaphore_wait(barrier, 7)

        step(x_copy, 0, "start")
        step(w13_copy, 0, "start")
        step(w2_copy, 0, "start")
        step(x_copy, 0, "recv")
        step(x_copy, 1, "start")
        step(w13_copy, 0, "recv")
        step(w13_copy, 1, "start")
        step(x_copy, 1, "recv")
        step(x_copy, 2, "start")
        step(w2_copy, 0, "recv")
        step(w2_copy, 1, "start")
        step(w13_copy, 1, "recv")
        step(w13_copy, 2, "start")
        step(x_copy, 2, "recv")
        for m in range(2):
            x_swap(m).start()
        for m in range(2):
            x_swap(m).wait_recv()
        step(w2_copy, 1, "recv")
        step(w2_copy, 2, "start")

        block = 4 * tok
        lane = lax.broadcasted_iota(jnp.int32, (block, 2 * LANES), 1)
        token = lax.broadcasted_iota(jnp.int32, (block, 2 * LANES), 0)
        per = 4 * cap
        span = experts_here * per
        part = lane // span
        in_part = lane % span
        near_expert = place + CUBE * (in_part // per)
        expert = core * n_local + near_expert + jnp.where(near_expert >= n_local, 1000, 0)
        key_of = jnp.where((in_part % per) // cap == token // tok, expert * cap + in_part % cap, -5).astype(F32)
        for m in range(2):
            for b in range(4):
                meta = xg[m, b * block:(b + 1) * block, dim:dim + LANES].astype(F32)
                hit = jnp.zeros((block, 2 * LANES), F32)
                gate = jnp.zeros((block, 2 * LANES), F32)
                for k in range(4):
                    same = meta[:, k:k + 1] == key_of
                    g = jnp.where(part == 0, meta[:, 4 + k:5 + k],
                                  jnp.where(part == 1, meta[:, 8 + k:9 + k], jnp.where(part == 2, meta[:, 12 + k:13 + k], 0.0)))
                    hit = jnp.where(same, 1.0, hit)
                    gate = jnp.where(same, g, gate)
                gm[m * 4 + b] = gate.astype(BF16)
                put = hit[:, :span].astype(BF16)
                rows = lax.dot_general(put, xg[m, b * block:(b + 1) * block, 0:dim], (((0,), (0,)), ((), ())),
                                       preferred_element_type=F32).astype(BF16)
                for j in range(experts_here):
                    r0 = (m * 4 + b) * per
                    xe[j, r0:r0 + per, :] = rows[j * per:(j + 1) * per]

        @pl.loop(0, experts_here)
        def _(j):
            slot = j % 2
            for c in routed_in(j):
                c.wait()
            for o in range(0, ff, CHUNK):
                n = min(CHUNK, ff - o)
                a = jnp.dot(xe[j], slots[slot, 0, :, o:o + n], preferred_element_type=F32)
                g = jnp.dot(xe[j], slots[slot, 1, :, o:o + n], preferred_element_type=F32)
                h[j, :, o:o + n] = (jax.nn.silu(a) * g).astype(BF16)

            @pl.when(j + 2 < experts_here)
            def _():
                for c in routed_in(j + 2):
                    c.start()

    pl.run_scoped(
        first_stage,
        pltpu.VMEM((2, 2, dim, ff), BF16),
        pltpu.VMEM((experts_here, 8 * 4 * cap, dim), BF16),
        pltpu.VMEM((dim, sff), BF16),
        pltpu.VMEM((dim, sff), BF16),
        pltpu.VMEM((sff, dim), BF16),
    )

    def second_stage(w2b, acc, sd, rr):
        def w2_in(n):
            cols = pl.ds(pl.multiple_of(n * CHUNK, CHUNK), CHUNK)
            return [pltpu.make_async_copy(rw2.at[expert_row(j), :, cols], w2b.at[n, j], w2_sem.at[n, j]) for j in range(experts_here)]

        @pl.loop(0, n_chunks)
        def _(n):
            for c in w2_in(n):
                c.start()

        rr[...] = jnp.zeros_like(rr)

        step(w13_copy, 2, "recv")
        rows = 2 * CUBE * tok // 2
        for m in range(2):
            @pl.loop(0, 2)
            def _(b):
                mine = pl.ds(pl.multiple_of(b * rows, rows), rows)
                x = xg[m, mine, 0:dim]
                a = lax.dot_general(x, wg13[m, 0], (((1,), (1,)), ((), ())), preferred_element_type=F32)
                g = lax.dot_general(x, wg13[m, 1], (((1,), (1,)), ((), ())), preferred_element_type=F32)
                hs[m, mine, :] = (jax.nn.silu(a) * g).astype(BF16)

        step(w2_copy, 2, "recv")

        block = 4 * tok
        per = 4 * cap
        span = experts_here * per
        full = CUBE * tok

        def d2d(n):
            return remote(sd.at[n], rd.at[n], rd_s.at[n], rd_r.at[n], partner)

        def halving(s, n, m, u):
            q = n * per_chunk + u
            rows = full >> (s + 1)
            dst = (r1, r2, r3)[s]
            return remote(acc.at[q, m, pl.ds(rows, rows)], dst.at[q, m], rs_s.at[s, q, m], rs_r.at[s, q, m], at(token_chip(m, (q + s) % 3)))

        def compute(n):
            for c in w2_in(n):
                c.wait()
            cols = pl.ds(pl.multiple_of(n * CHUNK, CHUNK), CHUNK)
            for j in range(experts_here):
                out = jnp.dot(h[j], w2b[n, j], preferred_element_type=F32).astype(BF16)
                for k in range(8):
                    for part in range(3):
                        r0 = part * span + j * per
                        rr[k, r0:r0 + per, :] = out[k * per:(k + 1) * per]
            lead = []
            for u in range(per_chunk):
                rho = (n * per_chunk + u) % 3
                lead.append([weight_of((i - rho + 3) % 3) for i in range(3)])
            for m in range(2):
                for b in range(4):
                    o = jnp.dot(hs[m, b * block:(b + 1) * block, :], wg2[m, :, cols], preferred_element_type=F32)
                    o += jnp.dot(gm[m * 4 + b], rr[m * 4 + b], preferred_element_type=F32)
                    for i in range(4):
                        r = (b % 2) * 4 + i
                        for u in range(per_chunk):
                            pos = sum(lead[u][bit] for bit in range(3) if r >> bit & 1)
                            where = pl.ds(pl.multiple_of(pos * tok, tok), tok) if r else pl.ds(0, tok)
                            piece = o[i * tok:(i + 1) * tok, u * LANES:(u + 1) * LANES]
                            if b < 2:
                                acc[n * per_chunk + u, m, where, :] = piece
                            else:
                                sd[n, m, u, where, :] = piece
            d2d(n).start()

        def each(n, f):
            for u in range(per_chunk):
                for m in range(2):
                    f(n * per_chunk + u, m, u)

        def from_partner(n):
            d2d(n).wait_recv()

            def f(q, m, u):
                acc[q, m] += rd[n, m, u]
                halving(0, n, m, u).start()
            each(n, f)

        def from_neighbour(s, n):
            def f(q, m, u):
                halving(s, n, m, u).wait_recv()
                rows = full >> (s + 1)
                acc[q, m, 0:rows, :] += (r1, r2)[s][q, m]
                halving(s + 1, n, m, u).start()
            each(n, f)

        def finish(n):
            def f(q, m, u):
                halving(2, n, m, u).wait_recv()
                cols = pl.ds(pl.multiple_of(q * LANES, LANES), LANES)
                y = acc[q, m, 0:tok, :] + r3[q, m] + xg[m, 0:tok, cols].astype(F32)
                (oa, ob)[m][:, cols] = y.astype(BF16)
            each(n, f)

        stages = [(0, compute), (1, from_partner), (3, functools.partial(from_neighbour, 0)), (5, functools.partial(from_neighbour, 1)), (7, finish)]

        @pl.loop(0, n_chunks + 7)
        def _(t):
            for lag, f in stages:
                @pl.when((t >= lag) & (t < n_chunks + lag))
                def _(lag=lag, f=f):
                    f(t - lag)

        @pl.loop(0, n_chunks)
        def _(n):
            d2d(n).wait_send()
            for s in range(3):
                each(n, lambda q, m, u: halving(s, n, m, u).wait_send())

    pl.run_scoped(
        second_stage,
        pltpu.VMEM((n_chunks, experts_here, ff, CHUNK), BF16),
        pltpu.VMEM((n_chunks * per_chunk, 2, CUBE * tok, LANES), F32),
        pltpu.VMEM((n_chunks, 2, per_chunk, CUBE * tok, LANES), F32),
        pltpu.VMEM((8, 2 * LANES, CHUNK), BF16),
    )

    for s in range(3):
        step(x_copy, s, "send")
        step(w13_copy, s, "send")
        step(w2_copy, s, "send")
    for m in range(2):
        x_swap(m).wait_send()


def routing_meta(expert_ids, gate_vals, slot_ids, cap):
    key = jnp.where(slot_ids >= 0, expert_ids * cap + slot_ids, -1).astype(F32)
    top = jnp.minimum(lax.reduce_precision(gate_vals, 8, 7), float(jnp.finfo(BF16).max))
    mid = lax.reduce_precision(gate_vals - top, 8, 7)
    low = lax.reduce_precision(gate_vals - top - mid, 8, 7)
    meta = jnp.concatenate([key, top, mid, low], axis=1)
    return jnp.pad(meta, ((0, 0), (0, LANES - meta.shape[1]))).astype(BF16)


def solution(mesh):
    ep_size = mesh.shape['ep']
    tok_spec = P(('data', 'ep', 'tp'), None)
    in_specs = (tok_spec,) * 8 + (P(None, 'tp'), P(None, 'tp'), P('tp', None), P('ep', None, None), P('ep', None, None), P('ep', None, None))

    def layer_local(tokens_a, tokens_b, experts_a, experts_b, gates_a, gates_b, slots_a, slots_b, shared_w1, shared_w3, shared_w2, routed_w1, routed_w3, routed_w2):
        tok, dim = tokens_a.shape
        n_local, _, ff = routed_w1.shape
        sff = shared_w1.shape[1]
        cap = capacity_rows(tok, experts_a.shape[1], n_local * ep_size)
        experts_here = -(-n_local // CUBE)
        cfg = dict(tok=tok, dim=dim, ff=ff, sff=sff, n_local=n_local, cap=cap, experts_here=experts_here, width=CUBE * HALF)
        meta_a = routing_meta(experts_a, gates_a, slots_a, cap)
        meta_b = routing_meta(experts_b, gates_b, slots_b, cap)
        n_chunks = dim // CHUNK
        n_q = dim // LANES
        dma = pltpu.SemaphoreType.DMA
        any_spec = pl.BlockSpec(memory_space=pl.ANY)
        return pl.pallas_call(
            functools.partial(kernel, cfg),
            out_shape=[jax.ShapeDtypeStruct((tok, dim), BF16)] * 2,
            in_specs=[any_spec] * 10,
            out_specs=[pl.BlockSpec(memory_space=pltpu.VMEM)] * 2,
            scratch_shapes=[
                pltpu.VMEM((2, 2 * CUBE * tok, dim + LANES), BF16),
                pltpu.VMEM((2, 2, CUBE * HALF, dim), BF16),
                pltpu.VMEM((2, CUBE * HALF, dim), BF16),
                pltpu.VMEM((experts_here, 8 * 4 * cap, ff), BF16),
                pltpu.VMEM((2, 2 * CUBE * tok, CUBE * HALF), BF16),
                pltpu.VMEM((8, 4 * tok, 2 * LANES), BF16),
                pltpu.VMEM((n_chunks, 2, CHUNK // LANES, CUBE * tok, LANES), F32),
                pltpu.VMEM((n_q, 2, CUBE * tok // 2, LANES), F32),
                pltpu.VMEM((n_q, 2, CUBE * tok // 4, LANES), F32),
                pltpu.VMEM((n_q, 2, CUBE * tok // 8, LANES), F32),
                dma((8,)),
                dma((2, 2)),
                dma((n_chunks, experts_here)),
                dma((2, 3, CUBE)), dma((2, 3, CUBE)),
                dma((2, 3, CUBE)), dma((2, 3, CUBE)),
                dma((2, 3, CUBE)), dma((2, 3, CUBE)),
                dma((2,)), dma((2,)),
                dma((n_chunks,)), dma((n_chunks,)),
                dma((3, n_q, 2)), dma((3, n_q, 2)),
            ],
            compiler_params=pltpu.CompilerParams(collective_id=0, has_side_effects=True, vmem_limit_bytes=67043328),
            name="expert_layer",
        )(tokens_a, tokens_b, meta_a, meta_b, shared_w1, shared_w3, shared_w2, routed_w1, routed_w3, routed_w2)

    return jax.shard_map(layer_local, mesh=mesh, in_specs=in_specs, out_specs=(tok_spec, tok_spec), check_vma=False)
```

```python
import functools

import jax
import jax.numpy as jnp
from jax import lax
from jax.experimental import pallas as pl
from jax.experimental.pallas import tpu as pltpu
from jax.sharding import PartitionSpec as P

MESH = pl.DeviceIdType.MESH
BF16 = jnp.bfloat16
F32 = jnp.float32
LANES = 128
CHUNK = 256
STRIDE = (1, 4, 16)
SIDE = 4
CUBE = 8
HALF = 48


def capacity_rows(tok_local, top_k, num_experts):
    return max(4, (2 * tok_local * top_k) // num_experts)


def column_parts(width, order):
    tiles = width // LANES
    size = [tiles // 3] * 3
    for i in range(tiles % 3):
        size[order[i]] += 1
    starts = [0, size[0], size[0] + size[1]]
    return [(s * LANES, n * LANES) for s, n in zip(starts, size)]


def weight_of(t):
    return 4 - 2 * t + (t * (t - 1)) // 2


def kernel(cfg, ta, tb, ea, eb, ga, gb, sa, sb, w1, w3, w2, rw1, rw3, rw2, oa, ob,
           xg, wg13, wg2, h, hs, gm, rd, r1, r2, r3,
           loc_sem, wl_sem, w2_sem, ag_s, ag_r, g13_s, g13_r, g2_s, g2_r, xd_s, xd_r, rd_s, rd_r, rs_s, rs_r):
    tok, dim, ff, sff, n_local, cap = (cfg[k] for k in ("tok", "dim", "ff", "sff", "n_local", "cap"))
    second_half = sff - HALF
    experts_here = cfg["experts_here"]
    n_chunks = dim // CHUNK
    per_chunk = CHUNK // LANES
    xcols = column_parts(dim + LANES, (0, 2, 1))
    wcols = column_parts(dim, (1, 0, 2))

    tp = lax.axis_index("tp")
    core = lax.axis_index("ep")
    coord = [tp % SIDE, (tp // SIDE) % SIDE, tp // (SIDE * SIDE)]
    near = [[tp + (1 - 2 * (c % 2)) * s for c, s in zip(coord, STRIDE)],
            [tp + (3 - 2 * c) * s for c, s in zip(coord, STRIDE)]]
    place = coord[0] % 2 + 2 * (coord[1] % 2) + 4 * (coord[2] % 2)

    def at(chip):
        return {"tp": chip, "ep": core}

    partner = {"tp": tp, "ep": 1 - core}

    def token_chip(m, d):
        n0, n1, n2 = near[m]
        return n0 + d * (n1 - n0) + ((d * (d - 1)) // 2) * (n2 - 2 * n1 + n0)

    def remote(src, dst, s, r, where):
        return pltpu.make_async_remote_copy(src_ref=src, dst_ref=dst, send_sem=s, recv_sem=r, device_id=where, device_id_type=MESH)

    def items_of(p, s):
        got = [0]
        for t in range(s):
            got = got + [i | (1 << ((p + t) % 3)) for i in got]
        return got

    def x_copy(m, p, s, i):
        d = (p + s) % 3
        to = i | (1 << d)
        c0, n = xcols[p]
        return remote(xg.at[m, pl.ds(i * tok, tok), pl.ds(c0, n)], xg.at[m, pl.ds(to * tok, tok), pl.ds(c0, n)],
                      ag_s.at[m], ag_r.at[m, p, to], at(near[m][d]))

    def w13_copy(m, p, s, i):
        d = (p + s) % 3
        to = i | (1 << d)
        c0, n = wcols[p]
        return remote(wg13.at[m, :, pl.ds(i * HALF, HALF), pl.ds(c0, n)], wg13.at[m, :, pl.ds(to * HALF, HALF), pl.ds(c0, n)],
                      g13_s.at[m], g13_r.at[m, p, to], at(near[1 - m][d]))

    def w2_copy(m, p, s, i):
        d = (p + s) % 3
        to = i | (1 << d)
        c0, n = wcols[p]
        return remote(wg2.at[m, pl.ds(i * HALF, HALF), pl.ds(c0, n)], wg2.at[m, pl.ds(to * HALF, HALF), pl.ds(c0, n)],
                      g2_s.at[m], g2_r.at[m, p, to], at(near[1 - m][d]))

    def step(copy, s, what):
        for m in range(2):
            for p in range(3):
                for i in items_of(p, s):
                    c = copy(m, p, s, i)
                    if what == "start":
                        c.start()
                    else:
                        c.wait_recv()

    def all_sent(ref, sem):
        pltpu.make_async_copy(ref, ref, sem).wait()

    half_rows = CUBE * tok

    def x_swap(m):
        return remote(xg.at[m, pl.ds(0, half_rows)], xg.at[m, pl.ds(half_rows, half_rows)], xd_s.at[m], xd_r.at[m], partner)

    barrier = pltpu.get_barrier_semaphore()
    for kind in range(2):
        for d in range(3):
            pl.semaphore_signal(barrier, inc=1, device_id=at(near[kind][d]), device_id_type=MESH)
    pl.semaphore_signal(barrier, inc=1, device_id=partner, device_id_type=MESH)

    half = pl.ds(pl.multiple_of(second_half * core, 8), HALF)
    own = [pltpu.make_async_copy(t, xg.at[m, pl.ds(0, tok), pl.ds(0, dim)], loc_sem.at[m]) for m, t in enumerate((ta, tb))]
    shared_in = []
    for m in range(2):
        shared_in.append(pltpu.make_async_copy(w1.at[half], wg13.at[m, 0, pl.ds(0, HALF)], loc_sem.at[2 + 3 * m]))
        shared_in.append(pltpu.make_async_copy(w3.at[half], wg13.at[m, 1, pl.ds(0, HALF)], loc_sem.at[3 + 3 * m]))
        shared_in.append(pltpu.make_async_copy(w2.at[half], wg2.at[m, pl.ds(0, HALF)], loc_sem.at[4 + 3 * m]))

    def expert_row(j):
        return (place + CUBE * j) % n_local

    def first_stage(slots, xe):
        def routed_in(j):
            e = expert_row(j)
            slot = j % 2
            return [pltpu.make_async_copy(src.at[e], slots.at[slot, k], wl_sem.at[slot, k]) for k, src in enumerate((rw1, rw3))]

        with jax.named_scope("load"):
            for c in own + shared_in:
                c.start()
            for j in range(2):
                for c in routed_in(j):
                    c.start()

            field = lax.broadcasted_iota(jnp.int32, (4, LANES), 1) - lax.broadcasted_iota(jnp.int32, (4, LANES), 0)
            for m, (e, g, sl) in enumerate(((ea, ga, sa), (eb, gb, sb))):
                key = jnp.where(sl[...] >= 0, e[...] * cap + sl[...], -1).astype(F32)
                gate = g[...]
                top = jnp.minimum(gate, float(jnp.finfo(BF16).max)).astype(BF16).astype(F32)
                mid = (gate - top).astype(BF16).astype(F32)
                low = gate - top - mid
                meta = jnp.zeros((tok, LANES), F32)
                for k, v in enumerate((key, top, mid, low)):
                    put = (field == 4 * k).astype(F32)
                    meta += lax.dot_general(v, put, (((0,), (0,)), ((), ())), preferred_element_type=F32)
                xg[m, 0:tok, dim:dim + LANES] = meta.astype(BF16)

            for c in own + shared_in:
                c.wait()
            over = 2 * HALF - sff
            tile = 16
            keep = (lax.broadcasted_iota(jnp.int32, (tile, dim), 0) >= over * core)
            for m in range(2):
                wg2[m, 0:tile, :] = jnp.where(keep, wg2[m, 0:tile, :].astype(F32), 0.0).astype(BF16)

        with jax.named_scope("barrier"):
            pl.semaphore_wait(barrier, 7)

        with jax.named_scope("first"):
            step(x_copy, 0, "start")
            step(w13_copy, 0, "start")
            step(w2_copy, 0, "start")
        with jax.named_scope("x0"):
            step(x_copy, 0, "recv")
        step(x_copy, 1, "start")
        with jax.named_scope("v0"):
            step(w13_copy, 0, "recv")
        step(w13_copy, 1, "start")
        with jax.named_scope("x1"):
            step(x_copy, 1, "recv")
        step(x_copy, 2, "start")
        with jax.named_scope("w0"):
            step(w2_copy, 0, "recv")
        step(w2_copy, 1, "start")
        with jax.named_scope("v1"):
            step(w13_copy, 1, "recv")
        step(w13_copy, 2, "start")
        with jax.named_scope("x2"):
            step(x_copy, 2, "recv")
        with jax.named_scope("swap"):
            for m in range(2):
                x_swap(m).start()
            for m in range(2):
                x_swap(m).wait_recv()
        with jax.named_scope("w1"):
            step(w2_copy, 1, "recv")
        step(w2_copy, 2, "start")

        block = 4 * tok
        lane = lax.broadcasted_iota(jnp.int32, (block, 2 * LANES), 1)
        token = lax.broadcasted_iota(jnp.int32, (block, 2 * LANES), 0)
        per = 4 * cap
        span = experts_here * per
        part = lane // span
        in_part = lane % span
        near_expert = place + CUBE * (in_part // per)
        expert = core * n_local + near_expert + jnp.where(near_expert >= n_local, 1000, 0)
        key_of = jnp.where((in_part % per) // cap == token // tok, expert * cap + in_part % cap, -5).astype(F32)
        for m in range(2):
            for b in range(4):
                meta = xg[m, b * block:(b + 1) * block, dim:dim + LANES].astype(F32)
                hit = jnp.zeros((block, 2 * LANES), F32)
                gate = jnp.zeros((block, 2 * LANES), F32)
                for k in range(4):
                    same = meta[:, k:k + 1] == key_of
                    g = jnp.where(part == 0, meta[:, 4 + k:5 + k],
                                  jnp.where(part == 1, meta[:, 8 + k:9 + k], jnp.where(part == 2, meta[:, 12 + k:13 + k], 0.0)))
                    hit = jnp.where(same, 1.0, hit)
                    gate = jnp.where(same, g, gate)
                gm[m * 4 + b] = gate.astype(BF16)
                put = hit[:, :span].astype(BF16)
                rows = lax.dot_general(put, xg[m, b * block:(b + 1) * block, 0:dim], (((0,), (0,)), ((), ())),
                                       preferred_element_type=F32).astype(BF16)
                for j in range(experts_here):
                    r0 = (m * 4 + b) * per
                    xe[j, r0:r0 + per, :] = rows[j * per:(j + 1) * per]

        @pl.loop(0, experts_here)
        def _(j):
            slot = j % 2
            with jax.named_scope("rwait"):
                for c in routed_in(j):
                    c.wait()
            with jax.named_scope("routed"):
                for o in range(0, ff, CHUNK):
                    n = min(CHUNK, ff - o)
                    a = jnp.dot(xe[j], slots[slot, 0, :, o:o + n], preferred_element_type=F32)
                    g = jnp.dot(xe[j], slots[slot, 1, :, o:o + n], preferred_element_type=F32)
                    h[j, :, o:o + n] = (jax.nn.silu(a) * g).astype(BF16)

            @pl.when(j + 2 < experts_here)
            def _():
                for c in routed_in(j + 2):
                    c.start()

    pl.run_scoped(
        first_stage,
        pltpu.VMEM((2, 2, dim, ff), BF16),
        pltpu.VMEM((experts_here, 8 * 4 * cap, dim), BF16),
    )

    def second_stage(w2b, acc, sd, rr):
        def w2_in(n):
            cols = pl.ds(pl.multiple_of(n * CHUNK, CHUNK), CHUNK)
            return [pltpu.make_async_copy(rw2.at[expert_row(j), :, cols], w2b.at[n, j], w2_sem.at[n, j]) for j in range(experts_here)]

        @pl.loop(0, n_chunks)
        def _(n):
            for c in w2_in(n):
                c.start()

        rr[...] = jnp.zeros_like(rr)

        with jax.named_scope("v2"):
            step(w13_copy, 2, "recv")
        rows = 2 * CUBE * tok // 2
        for m in range(2):
            @pl.loop(0, 2)
            def _(b):
                mine = pl.ds(pl.multiple_of(b * rows, rows), rows)
                x = xg[m, mine, 0:dim]
                a = lax.dot_general(x, wg13[m, 0], (((1,), (1,)), ((), ())), preferred_element_type=F32)
                g = lax.dot_general(x, wg13[m, 1], (((1,), (1,)), ((), ())), preferred_element_type=F32)
                hs[m, mine, :] = (jax.nn.silu(a) * g).astype(BF16)

        with jax.named_scope("w2"):
            step(w2_copy, 2, "recv")
            rest = CUBE - 1
            for m in range(2):
                all_sent(xg.at[m, pl.ds(0, rest * tok)], ag_s.at[m])
                all_sent(wg13.at[m, :, pl.ds(0, rest * HALF)], g13_s.at[m])
                all_sent(wg2.at[m, pl.ds(0, rest * HALF)], g2_s.at[m])
                x_swap(m).wait_send()

        block = 4 * tok
        per = 4 * cap
        span = experts_here * per
        full = CUBE * tok

        def d2d(n):
            return remote(sd.at[n], rd.at[n], rd_s, rd_r.at[n], partner)

        def halving(s, n, m, u):
            q = n * per_chunk + u
            rows = full >> (s + 1)
            dst = (r1, r2, r3)[s]
            return remote(acc.at[q, m, pl.ds(rows, rows)], dst.at[q, m], rs_s.at[m], rs_r.at[s, q, m], at(token_chip(m, (q + s) % 3)))

        def compute(n):
            for c in w2_in(n):
                c.wait()
            cols = pl.ds(pl.multiple_of(n * CHUNK, CHUNK), CHUNK)
            for j in range(experts_here):
                out = jnp.dot(h[j], w2b[n, j], preferred_element_type=F32).astype(BF16)
                for k in range(8):
                    for part in range(3):
                        r0 = part * span + j * per
                        rr[k, r0:r0 + per, :] = out[k * per:(k + 1) * per]
            lead = []
            for u in range(per_chunk):
                rho = (n * per_chunk + u) % 3
                lead.append([weight_of((i - rho + 3) % 3) for i in range(3)])
            for m in range(2):
                for b in range(4):
                    o = jnp.dot(hs[m, b * block:(b + 1) * block, :], wg2[m, :, cols], preferred_element_type=F32)
                    o += jnp.dot(gm[m * 4 + b], rr[m * 4 + b], preferred_element_type=F32)
                    for i in range(4):
                        r = (b % 2) * 4 + i
                        for u in range(per_chunk):
                            pos = sum(lead[u][bit] for bit in range(3) if r >> bit & 1)
                            where = pl.ds(pl.multiple_of(pos * tok, tok), tok) if r else pl.ds(0, tok)
                            piece = o[i * tok:(i + 1) * tok, u * LANES:(u + 1) * LANES]
                            if b < 2:
                                acc[n * per_chunk + u, m, where, :] = piece
                            else:
                                sd[n, m, u, where, :] = piece
            d2d(n).start()

        def each(n, f):
            for u in range(per_chunk):
                for m in range(2):
                    f(n * per_chunk + u, m, u)

        def from_partner(n):
            d2d(n).wait_recv()

            def f(q, m, u):
                acc[q, m] += rd[n, m, u]
                halving(0, n, m, u).start()
            each(n, f)

        def from_neighbour(s, n):
            def f(q, m, u):
                halving(s, n, m, u).wait_recv()
                rows = full >> (s + 1)
                acc[q, m, 0:rows, :] += (r1, r2)[s][q, m]
                halving(s + 1, n, m, u).start()
            each(n, f)

        def finish(n):
            def f(q, m, u):
                halving(2, n, m, u).wait_recv()
                cols = pl.ds(pl.multiple_of(q * LANES, LANES), LANES)
                y = acc[q, m, 0:tok, :] + r3[q, m] + xg[m, 0:tok, cols].astype(F32)
                (oa, ob)[m][:, cols] = y.astype(BF16)
            each(n, f)

        stages = [(0, compute), (1, from_partner), (3, functools.partial(from_neighbour, 0)), (5, functools.partial(from_neighbour, 1)), (7, finish)]

        @pl.loop(0, n_chunks + 7)
        def _(t):
            for lag, f in stages:
                @pl.when((t >= lag) & (t < n_chunks + lag))
                def _(lag=lag, f=f):
                    with jax.named_scope(f"s{lag}"):
                        f(t - lag)

        with jax.named_scope("sent"):
            all_sent(sd, rd_s)
            for m in range(2):
                all_sent(acc.at[:, m, pl.ds(0, full - tok)], rs_s.at[m])

    pl.run_scoped(
        second_stage,
        pltpu.VMEM((n_chunks, experts_here, ff, CHUNK), BF16),
        pltpu.VMEM((n_chunks * per_chunk, 2, CUBE * tok, LANES), F32),
        pltpu.VMEM((n_chunks, 2, per_chunk, CUBE * tok, LANES), F32),
        pltpu.VMEM((8, 2 * LANES, CHUNK), BF16),
    )


def solution(mesh):
    ep_size = mesh.shape['ep']
    tok_spec = P(('data', 'ep', 'tp'), None)
    in_specs = (tok_spec,) * 8 + (P(None, 'tp'), P(None, 'tp'), P('tp', None), P('ep', None, None), P('ep', None, None), P('ep', None, None))

    def layer_local(tokens_a, tokens_b, experts_a, experts_b, gates_a, gates_b, slots_a, slots_b, shared_w1, shared_w3, shared_w2, routed_w1, routed_w3, routed_w2):
        tok, dim = tokens_a.shape
        n_local, _, ff = routed_w1.shape
        sff = shared_w1.shape[1]
        cap = capacity_rows(tok, experts_a.shape[1], n_local * ep_size)
        experts_here = -(-n_local // CUBE)
        cfg = dict(tok=tok, dim=dim, ff=ff, sff=sff, n_local=n_local, cap=cap, experts_here=experts_here)
        n_chunks = dim // CHUNK
        n_q = dim // LANES
        dma = pltpu.SemaphoreType.DMA
        any_spec = pl.BlockSpec(memory_space=pl.ANY)
        vmem_spec = pl.BlockSpec(memory_space=pltpu.VMEM)
        return pl.pallas_call(
            functools.partial(kernel, cfg),
            out_shape=[pltpu.VMEM((tok, dim), BF16)] * 2,
            in_specs=[any_spec] * 2 + [vmem_spec] * 6 + [any_spec] * 6,
            out_specs=[vmem_spec] * 2,
            scratch_shapes=[
                pltpu.VMEM((2, 2 * CUBE * tok, dim + LANES), BF16),
                pltpu.VMEM((2, 2, CUBE * HALF, dim), BF16),
                pltpu.VMEM((2, CUBE * HALF, dim), BF16),
                pltpu.VMEM((experts_here, 8 * 4 * cap, ff), BF16),
                pltpu.VMEM((2, 2 * CUBE * tok, CUBE * HALF), BF16),
                pltpu.VMEM((8, 4 * tok, 2 * LANES), BF16),
                pltpu.VMEM((n_chunks, 2, CHUNK // LANES, CUBE * tok, LANES), F32),
                pltpu.VMEM((n_q, 2, CUBE * tok // 2, LANES), F32),
                pltpu.VMEM((n_q, 2, CUBE * tok // 4, LANES), F32),
                pltpu.VMEM((n_q, 2, CUBE * tok // 8, LANES), F32),
                dma((8,)),
                dma((2, 2)),
                dma((n_chunks, experts_here)),
                dma((2,)), dma((2, 3, CUBE)),
                dma((2,)), dma((2, 3, CUBE)),
                dma((2,)), dma((2, 3, CUBE)),
                dma((2,)), dma((2,)),
                dma(()), dma((n_chunks,)),
                dma((2,)), dma((3, n_q, 2)),
            ],
            compiler_params=pltpu.CompilerParams(collective_id=0, has_side_effects=True, vmem_limit_bytes=60 * 2**20),
            name="expert_layer",
        )(tokens_a, tokens_b, experts_a.T, experts_b.T, gates_a.T, gates_b.T, slots_a.T, slots_b.T,
          shared_w1.T, shared_w3.T, shared_w2, routed_w1, routed_w3, routed_w2)

    return jax.shard_map(layer_local, mesh=mesh, in_specs=in_specs, out_specs=(tok_spec, tok_spec), check_vma=False)
```

```python
import functools

import jax
import jax.numpy as jnp
from jax import lax
from jax.experimental import pallas as pl
from jax.experimental.pallas import tpu as pltpu
from jax.sharding import PartitionSpec as P

MESH = pl.DeviceIdType.MESH
BF16 = jnp.bfloat16
F32 = jnp.float32
LANES = 128
CHUNK = 256
STRIDE = (1, 4, 16)
SIDE = 4
CUBE = 8
HALF = 48
SUB = 16
EARLY = 128


def capacity_rows(tok_local, top_k, num_experts):
    return max(4, (2 * tok_local * top_k) // num_experts)


def column_parts(width, order):
    tiles = width // LANES
    size = [tiles // 3] * 3
    for i in range(tiles % 3):
        size[order[i]] += 1
    starts = [0, size[0], size[0] + size[1]]
    return [(s * LANES, n * LANES) for s, n in zip(starts, size)]


def weight_of(t):
    return 4 - 2 * t + (t * (t - 1)) // 2


def kernel(cfg, ta, tb, ea, eb, ga, gb, sa, sb, w1, w3, w2, rw1, rw3, rw2, oa, ob,
           xg, wg13, wg2, h, hs, gm, rd, r1, r2, r3,
           loc_sem, wl_sem, w2_sem, ag_s, ag_r, g13_s, g13_r, g2_s, g2_r, xd_s, xd_r, rd_s, rd_r, rs_s, rs_r):
    tok, dim, ff, sff, n_local, cap = (cfg[k] for k in ("tok", "dim", "ff", "sff", "n_local", "cap"))
    second_half = sff - HALF
    experts_here = cfg["experts_here"]
    n_chunks = dim // CHUNK
    per_chunk = CHUNK // LANES
    xcols = column_parts(dim + LANES, (0, 2, 1))

    tp = lax.axis_index("tp")
    core = lax.axis_index("ep")
    coord = [tp % SIDE, (tp // SIDE) % SIDE, tp // (SIDE * SIDE)]
    near = [[tp + (1 - 2 * (c % 2)) * s for c, s in zip(coord, STRIDE)],
            [tp + (3 - 2 * c) * s for c, s in zip(coord, STRIDE)]]
    place = coord[0] % 2 + 2 * (coord[1] % 2) + 4 * (coord[2] % 2)

    def at(chip):
        return {"tp": chip, "ep": core}

    partner = {"tp": tp, "ep": 1 - core}

    def token_chip(m, d):
        n0, n1, n2 = near[m]
        return n0 + d * (n1 - n0) + ((d * (d - 1)) // 2) * (n2 - 2 * n1 + n0)

    def remote(src, dst, s, r, where):
        return pltpu.make_async_remote_copy(src_ref=src, dst_ref=dst, send_sem=s, recv_sem=r, device_id=where, device_id_type=MESH)

    def items_of(p, s):
        got = [0]
        for t in range(s):
            got = got + [i | (1 << ((p + t) % 3)) for i in got]
        return got

    def x_copy(m, p, s, i):
        d = (p + s) % 3
        to = i | (1 << d)
        c0, n = xcols[p]
        return remote(xg.at[m, pl.ds(i * tok, tok), pl.ds(c0, n)], xg.at[m, pl.ds(to * tok, tok), pl.ds(c0, n)],
                      ag_s, ag_r.at[s], at(near[m][d]))

    def weight_row(p, t):
        return p * 4 * SUB + t * SUB if t < 4 else 3 * 4 * SUB + p * 4 * SUB + (t - 4) * SUB

    def w13_copy(m, p, s):
        rows = SUB << s
        return remote(wg13.at[m, :, pl.ds(weight_row(p, 0), rows)], wg13.at[m, :, pl.ds(weight_row(p, 1 << s), rows)],
                      g13_s, g13_r.at[s], at(near[1 - m][(p + s) % 3]))

    wave = dim // 2

    def w2_copy(k, m, p, s):
        rows, cols = SUB << s, pl.ds(k * wave, wave)
        return remote(wg2.at[m, pl.ds(weight_row(p, 0), rows), cols], wg2.at[m, pl.ds(weight_row(p, 1 << s), rows), cols],
                      g2_s, g2_r.at[k, s], at(near[1 - m][(p + s) % 3]))

    def settle(ref, sem):
        pltpu.make_async_copy(ref, ref, sem).wait()

    def send_x(s):
        for m in range(2):
            for p in range(3):
                for i in items_of(p, s):
                    x_copy(m, p, s, i).start()

    def settle_x(s):
        settle(xg.at[:, pl.ds(0, tok << s)], ag_r.at[s])

    def send_w13(s):
        for m in range(2):
            for p in range(3):
                w13_copy(m, p, s).start()

    def settle_w13(s):
        settle(wg13.at[:, :, pl.ds(0, HALF << s)], g13_r.at[s])

    def send_w2(k, s):
        for m in range(2):
            for p in range(3):
                w2_copy(k, m, p, s).start()

    def settle_w2(k, s):
        settle(wg2.at[:, pl.ds(0, HALF << s), pl.ds(0, wave)], g2_r.at[k, s])

    half_rows = CUBE * tok

    def x_swap(m):
        return remote(xg.at[m, pl.ds(0, half_rows)], xg.at[m, pl.ds(half_rows, half_rows)], xd_s, xd_r, partner)

    barrier = pltpu.get_barrier_semaphore()
    for kind in range(2):
        for d in range(3):
            pl.semaphore_signal(barrier, inc=1, device_id=at(near[kind][d]), device_id_type=MESH)
    pl.semaphore_signal(barrier, inc=1, device_id=partner, device_id_type=MESH)

    own = [pltpu.make_async_copy(t, xg.at[m, pl.ds(0, tok), pl.ds(0, dim)], loc_sem.at[0]) for m, t in enumerate((ta, tb))]
    shared_in = []
    for m in range(2):
        for p in range(3):
            src = pl.ds(pl.multiple_of(second_half * core + p * SUB, 8), SUB)
            dst = pl.ds(weight_row(p, 0), SUB)
            shared_in.append(pltpu.make_async_copy(w1.at[src], wg13.at[m, 0, dst], loc_sem.at[1]))
            shared_in.append(pltpu.make_async_copy(w3.at[src], wg13.at[m, 1, dst], loc_sem.at[1]))
            shared_in.append(pltpu.make_async_copy(w2.at[src], wg2.at[m, dst], loc_sem.at[1]))

    def expert_row(j):
        return (place + CUBE * j) % n_local

    def first_stage(slots, xe):
        def routed_in(j):
            e = expert_row(j)
            slot = j % 3
            return [pltpu.make_async_copy(src.at[e], slots.at[slot, k], wl_sem.at[slot]) for k, src in enumerate((rw1, rw3))]

        with jax.named_scope("load"):
            for c in own + shared_in:
                c.start()
            for j in range(3):
                for c in routed_in(j):
                    c.start()

            field = lax.broadcasted_iota(jnp.int32, (4, LANES), 1) - lax.broadcasted_iota(jnp.int32, (4, LANES), 0)
            for m, (e, g, sl) in enumerate(((ea, ga, sa), (eb, gb, sb))):
                key = jnp.where(sl[...] >= 0, e[...] * cap + sl[...], -1).astype(F32)
                gate = g[...]
                top = jnp.minimum(gate, float(jnp.finfo(BF16).max)).astype(BF16).astype(F32)
                mid = (gate - top).astype(BF16).astype(F32)
                low = gate - top - mid
                meta = jnp.zeros((tok, LANES), F32)
                for k, v in enumerate((key, top, mid, low)):
                    put = (field == 4 * k).astype(F32)
                    meta += lax.dot_general(v, put, (((0,), (0,)), ((), ())), preferred_element_type=F32)
                xg[m, 0:tok, dim:dim + LANES] = meta.astype(BF16)

            settle(xg.at[:, pl.ds(0, tok), pl.ds(0, dim)], loc_sem.at[0])
            settle(wg13.at[:, :, pl.ds(0, HALF)], loc_sem.at[1])
            settle(wg2.at[:, pl.ds(0, HALF)], loc_sem.at[1])
            over = 2 * HALF - sff
            tile = SUB
            keep = (lax.broadcasted_iota(jnp.int32, (tile, dim), 0) >= over * core)
            for m in range(2):
                wg2[m, 0:tile, :] = jnp.where(keep, wg2[m, 0:tile, :].astype(F32), 0.0).astype(BF16)

        with jax.named_scope("barrier"):
            pl.semaphore_wait(barrier, 7)

        with jax.named_scope("first"):
            send_x(0)
            send_w13(0)
            send_w2(0, 0)
            send_w2(1, 0)
        with jax.named_scope("x0"):
            settle_x(0)
        send_x(1)
        with jax.named_scope("v0"):
            settle_w13(0)
        send_w13(1)
        with jax.named_scope("x1"):
            settle_x(1)
        send_x(2)
        with jax.named_scope("v1"):
            settle_w13(1)
        send_w13(2)
        with jax.named_scope("x2"):
            settle_x(2)
        for m in range(2):
            x_swap(m).start()
        with jax.named_scope("a0"):
            settle_w2(0, 0)
        send_w2(0, 1)

        block = 4 * tok
        lane = lax.broadcasted_iota(jnp.int32, (block, 2 * LANES), 1)
        token = lax.broadcasted_iota(jnp.int32, (block, 2 * LANES), 0)
        per = 4 * cap
        span = experts_here * per
        part = lane // span
        in_part = lane % span
        near_expert = place + CUBE * (in_part // per)
        expert = core * n_local + near_expert + jnp.where(near_expert >= n_local, 1000, 0)
        key_of = jnp.where((in_part % per) // cap == token // tok, expert * cap + in_part % cap, -5).astype(F32)
        def build(b):
            for m in range(2):
                meta = xg[m, b * block:(b + 1) * block, dim:dim + LANES].astype(F32)
                hit = jnp.zeros((block, 2 * LANES), F32)
                gate = jnp.zeros((block, 2 * LANES), F32)
                for k in range(4):
                    same = meta[:, k:k + 1] == key_of
                    g = jnp.where(part == 0, meta[:, 4 + k:5 + k],
                                  jnp.where(part == 1, meta[:, 8 + k:9 + k], jnp.where(part == 2, meta[:, 12 + k:13 + k], 0.0)))
                    hit = jnp.where(same, 1.0, hit)
                    gate = jnp.where(same, g, gate)
                gm[m * 4 + b] = gate.astype(BF16)
                put = hit[:, :span].astype(BF16)
                rows = lax.dot_general(put, xg[m, b * block:(b + 1) * block, 0:dim], (((0,), (0,)), ((), ())),
                                       preferred_element_type=F32).astype(BF16)
                for j in range(experts_here):
                    r0 = (m * 4 + b) * per
                    xe[j, r0:r0 + per, :] = rows[j * per:(j + 1) * per]

        with jax.named_scope("build0"):
            build(0)
            build(1)
        with jax.named_scope("swap"):
            settle(xg.at[:, pl.ds(half_rows, half_rows)], xd_r)
        with jax.named_scope("build1"):
            build(2)
            build(3)

        @pl.loop(0, experts_here)
        def _(j):
            slot = j % 3

            @pl.when(j == 3)
            def _():
                with jax.named_scope("b0"):
                    settle_w2(1, 0)
                send_w2(1, 1)

            with jax.named_scope("rwait"):
                settle(slots.at[slot], wl_sem.at[slot])
            with jax.named_scope("routed"):
                for o in range(0, ff, CHUNK):
                    n = min(CHUNK, ff - o)
                    a = jnp.dot(xe[j], slots[slot, 0, :, o:o + n], preferred_element_type=F32)
                    g = jnp.dot(xe[j], slots[slot, 1, :, o:o + n], preferred_element_type=F32)
                    h[j, :, o:o + n] = (jax.nn.silu(a) * g).astype(BF16)

            @pl.when(j + 3 < experts_here)
            def _():
                for c in routed_in(j + 3):
                    c.start()

    pl.run_scoped(
        first_stage,
        pltpu.VMEM((3, 2, dim, ff), BF16),
        pltpu.VMEM((experts_here, 8 * 4 * cap, dim), BF16),
    )

    def second_stage(w2b, acc, sd, rr):
        def w2_in(n):
            cols = pl.ds(pl.multiple_of(n * CHUNK, CHUNK), CHUNK)
            return [pltpu.make_async_copy(rw2.at[expert_row(j), :, cols], w2b.at[n, j], w2_sem.at[n]) for j in range(experts_here)]

        @pl.loop(0, n_chunks)
        def _(n):
            for c in w2_in(n):
                c.start()

        rows = CUBE * tok

        def shared(lo, n):
            for m in range(2):
                @pl.loop(0, 2)
                def _(b):
                    mine = pl.ds(pl.multiple_of(b * rows, rows), rows)
                    x = xg[m, mine, 0:dim]
                    a = lax.dot_general(x, wg13[m, 0, lo:lo + n], (((1,), (1,)), ((), ())), preferred_element_type=F32)
                    g = lax.dot_general(x, wg13[m, 1, lo:lo + n], (((1,), (1,)), ((), ())), preferred_element_type=F32)
                    hs[m, mine, lo:lo + n] = (jax.nn.silu(a) * g).astype(BF16)

        with jax.named_scope("a1"):
            settle_w2(0, 1)
        send_w2(0, 2)
        with jax.named_scope("early"):
            shared(0, EARLY)
        with jax.named_scope("b1"):
            settle_w2(1, 1)
        send_w2(1, 2)
        with jax.named_scope("v2"):
            settle_w13(2)
        with jax.named_scope("late"):
            shared(EARLY, CUBE * HALF - EARLY)

        with jax.named_scope("w2"):
            settle_w2(0, 2)
            rest = CUBE - 1
            settle(xg.at[:, pl.ds(0, rest * tok)], ag_s)
            settle(wg13.at[:, :, pl.ds(0, rest * HALF)], g13_s)
            settle(xg.at[:, pl.ds(0, half_rows)], xd_s)
        rr[:, 3 * experts_here * 4 * cap:, :] = jnp.zeros((8, 2 * LANES - 3 * experts_here * 4 * cap, CHUNK), BF16)

        block = 4 * tok
        per = 4 * cap
        span = experts_here * per
        full = CUBE * tok

        def d2d(n):
            return remote(sd.at[n], rd.at[n], rd_s, rd_r.at[n], partner)

        def halving(s, n, m, u):
            q = n * per_chunk + u
            rows = full >> (s + 1)
            dst = (r1, r2, r3)[s]
            return remote(acc.at[q, m, pl.ds(rows, rows)], dst.at[q, m], rs_s, rs_r.at[s, n], at(token_chip(m, (q + s) % 3)))

        def compute(n):
            settle(w2b.at[n], w2_sem.at[n])

            @pl.when(n == n_chunks // 2)
            def _():
                settle_w2(1, 2)
                settle(wg2.at[:, pl.ds(0, (CUBE - 1) * HALF)], g2_s)

            cols = pl.ds(pl.multiple_of(n * CHUNK, CHUNK), CHUNK)
            for j in range(experts_here):
                out = jnp.dot(h[j], w2b[n, j], preferred_element_type=F32).astype(BF16)
                for k in range(8):
                    for part in range(3):
                        r0 = part * span + j * per
                        rr[k, r0:r0 + per, :] = out[k * per:(k + 1) * per]
            lead = []
            for u in range(per_chunk):
                rho = (n * per_chunk + u) % 3
                lead.append([weight_of((i - rho + 3) % 3) for i in range(3)])
            for m in range(2):
                for b in range(4):
                    o = jnp.dot(hs[m, b * block:(b + 1) * block, :], wg2[m, :, cols], preferred_element_type=F32)
                    o += jnp.dot(gm[m * 4 + b], rr[m * 4 + b], preferred_element_type=F32)
                    for i in range(4):
                        r = (b % 2) * 4 + i
                        for u in range(per_chunk):
                            pos = sum(lead[u][bit] for bit in range(3) if r >> bit & 1)
                            where = pl.ds(pl.multiple_of(pos * tok, tok), tok) if r else pl.ds(0, tok)
                            piece = o[i * tok:(i + 1) * tok, u * LANES:(u + 1) * LANES]
                            if b < 2:
                                acc[n * per_chunk + u, m, where, :] = piece
                            else:
                                sd[n, m, u, where, :] = piece
            d2d(n).start()

        def each(n, f):
            for u in range(per_chunk):
                for m in range(2):
                    f(n * per_chunk + u, m, u)

        def from_partner(n):
            settle(rd.at[n], rd_r.at[n])

            def f(q, m, u):
                acc[q, m] += rd[n, m, u]
                halving(0, n, m, u).start()
            each(n, f)

        def from_neighbour(s, n):
            settle((r1, r2)[s].at[pl.ds(n * per_chunk, per_chunk)], rs_r.at[s, n])

            def f(q, m, u):
                rows = full >> (s + 1)
                acc[q, m, 0:rows, :] += (r1, r2)[s][q, m]
                halving(s + 1, n, m, u).start()
            each(n, f)

        def finish(n):
            settle(r3.at[pl.ds(n * per_chunk, per_chunk)], rs_r.at[2, n])

            def f(q, m, u):
                cols = pl.ds(pl.multiple_of(q * LANES, LANES), LANES)
                y = acc[q, m, 0:tok, :] + r3[q, m] + xg[m, 0:tok, cols].astype(F32)
                (oa, ob)[m][:, cols] = y.astype(BF16)
            each(n, f)

        stages = [(0, compute), (2, from_partner), (6, functools.partial(from_neighbour, 0)), (8, functools.partial(from_neighbour, 1)), (12, finish)]

        @pl.loop(0, n_chunks + stages[-1][0])
        def _(t):
            for lag, f in stages:
                @pl.when((t >= lag) & (t < n_chunks + lag))
                def _(lag=lag, f=f):
                    with jax.named_scope(f"s{lag}"):
                        f(t - lag)

        with jax.named_scope("sent"):
            settle(sd, rd_s)
            settle(acc.at[:, :, pl.ds(0, full - tok)], rs_s)

    pl.run_scoped(
        second_stage,
        pltpu.VMEM((n_chunks, experts_here, ff, CHUNK), BF16),
        pltpu.VMEM((n_chunks * per_chunk, 2, CUBE * tok, LANES), F32),
        pltpu.VMEM((n_chunks, 2, per_chunk, CUBE * tok, LANES), F32),
        pltpu.VMEM((8, 2 * LANES, CHUNK), BF16),
    )


def solution(mesh):
    ep_size = mesh.shape['ep']
    tok_spec = P(('data', 'ep', 'tp'), None)
    in_specs = (tok_spec,) * 8 + (P(None, 'tp'), P(None, 'tp'), P('tp', None), P('ep', None, None), P('ep', None, None), P('ep', None, None))

    def layer_local(tokens_a, tokens_b, experts_a, experts_b, gates_a, gates_b, slots_a, slots_b, shared_w1, shared_w3, shared_w2, routed_w1, routed_w3, routed_w2):
        tok, dim = tokens_a.shape
        n_local, _, ff = routed_w1.shape
        sff = shared_w1.shape[1]
        cap = capacity_rows(tok, experts_a.shape[1], n_local * ep_size)
        experts_here = -(-n_local // CUBE)
        cfg = dict(tok=tok, dim=dim, ff=ff, sff=sff, n_local=n_local, cap=cap, experts_here=experts_here)
        n_chunks = dim // CHUNK
        n_q = dim // LANES
        dma = pltpu.SemaphoreType.DMA
        any_spec = pl.BlockSpec(memory_space=pl.ANY)
        vmem_spec = pl.BlockSpec(memory_space=pltpu.VMEM)
        return pl.pallas_call(
            functools.partial(kernel, cfg),
            out_shape=[pltpu.VMEM((tok, dim), BF16)] * 2,
            in_specs=[any_spec] * 2 + [vmem_spec] * 6 + [any_spec] * 6,
            out_specs=[vmem_spec] * 2,
            scratch_shapes=[
                pltpu.VMEM((2, 2 * CUBE * tok, dim + LANES), BF16),
                pltpu.VMEM((2, 2, CUBE * HALF, dim), BF16),
                pltpu.VMEM((2, CUBE * HALF, dim), BF16),
                pltpu.VMEM((experts_here, 8 * 4 * cap, ff), BF16),
                pltpu.VMEM((2, 2 * CUBE * tok, CUBE * HALF), BF16),
                pltpu.VMEM((8, 4 * tok, 2 * LANES), BF16),
                pltpu.VMEM((n_chunks, 2, CHUNK // LANES, CUBE * tok, LANES), F32),
                pltpu.VMEM((n_q, 2, CUBE * tok // 2, LANES), F32),
                pltpu.VMEM((n_q, 2, CUBE * tok // 4, LANES), F32),
                pltpu.VMEM((n_q, 2, CUBE * tok // 8, LANES), F32),
                dma((2,)),
                dma((3,)),
                dma((n_chunks,)),
                dma(()), dma((3,)),
                dma(()), dma((3,)),
                dma(()), dma((2, 3)),
                dma(()), dma(()),
                dma(()), dma((n_chunks,)),
                dma(()), dma((3, n_chunks)),
            ],
            compiler_params=pltpu.CompilerParams(collective_id=0, has_side_effects=True, vmem_limit_bytes=63 * 2**20),
            name="expert_layer",
        )(tokens_a, tokens_b, experts_a.T, experts_b.T, gates_a.T, gates_b.T, slots_a.T, slots_b.T,
          shared_w1.T, shared_w3.T, shared_w2, routed_w1, routed_w3, routed_w2)

    return jax.shard_map(layer_local, mesh=mesh, in_specs=in_specs, out_specs=(tok_spec, tok_spec), check_vma=False)
```
